32 devices in a mesh: rep: 4 (over y, x), tp: 8 (over z, core).
Axes of the slice: x: 2, y: 2, z: 4, core: 2. Of those that a mesh axis runs over, the one named last changes fastest.
Arguments:
- hidden: bfloat16 [2048, 14336], P('rep'), may hold values from -6 to 6
- ln_gain: float32 [14336], replicated, may hold values from 0.1 to 1.9
- ln_shift: float32 [14336], replicated, may hold values from -3 to 3
- qkv_weight: bfloat16 [14336, 16, 384], P(('rep', 'tp')), may hold values from -0.046875 to 0.046875
- qkv_bias: float32 [16, 384], P('tp'), may hold values from -64 to 64
- out_weight: bfloat16 [14336, 16, 128], P('tp'), may hold values from -0.375 to 0.375
- out_bias: float32 [14336], P('tp'), may hold values from -3 to 3
- slope_index: int32 [16], P('tp'), may hold values from 0 to 111
Outputs:
- attended: bfloat16 [2048, 14336], P('rep', 'tp')
The draws below stay inside these ranges and needn't reach their ends.
All inputs are finite; a program needn't handle non-finite values.
Results may differ from the reference program's by a relative error of at most 0.024.
The reference program's roundings to bfloat16 on the way count: a program that leaves them out, or rounds other values in their place, can miss the bound.
Values may be sent and summed in bfloat16 or wider, within the bound.
A program may use at most 192 MiB of HBM per device.

```python
import math
import jax
import jax.numpy as jnp
from jax import lax

D = 14336
N_SLOPES = 112
HEAD_DIM = 128
HEADS_DEV = 2
SEQ = 512
HEADS = 16
TOKENS = 2048
N_REP = 4


def draw_qkv_bias(key, part):
    base = 0.5 * jax.random.normal(key, (HEADS, 3 * HEAD_DIM), jnp.float32)
    return base


def plant(entries, rng, smallest, largest):
    place = [jax.random.randint(jax.random.fold_in(rng, axis), (), 0, length) for axis, length in enumerate(entries.shape)]
    longest = entries.shape.index(max(entries.shape))
    next_to = place[:longest] + [(place[longest] + 1) % entries.shape[longest]] + place[longest + 1:]
    return entries.at[tuple(place)].set(smallest).at[tuple(next_to)].set(largest)


def block_levels(rng, extent, cuts, low, high):
    factor_of, own = 1.0, jax.random.fold_in(rng, 6)
    for dim, blocks in cuts:
        heights = jnp.exp(jax.random.uniform(jax.random.fold_in(own, dim), (blocks,), jnp.float32, low / len(cuts), high / len(cuts)))
        factor_of = factor_of * jnp.repeat(heights, extent[dim] // blocks).reshape([-1 if axis == dim else 1 for axis in range(len(extent))])
    return factor_of


def gaussian(rng, shape, width, limit, cuts=(), held_as=jnp.bfloat16):
    result = width * jax.random.normal(rng, shape, jnp.float32)
    if cuts:
        result = result * block_levels(rng, shape, cuts, -0.22, 0.18)
    return jnp.clip(result, -limit, limit).astype(held_as)


def setup_inputs(seed: int = 0) -> dict:
    seeds = jax.random.split(jax.random.key(seed), 9)
    return {
        "hidden": gaussian(seeds[0], (TOKENS, D), 1.0, 6.0, ((0, 4),)),
        "ln_gain": jnp.clip(1.0 + 0.18 * jax.random.normal(seeds[1], (D,), jnp.float32), 0.1, 1.9),
        "ln_shift": gaussian(seeds[2], (D,), 0.5, 3.0, (), jnp.float32),
        "qkv_weight": gaussian(seeds[3], (D, HEADS, 3 * HEAD_DIM), D ** -0.5, 0.046875, ((0, 32),)),
        "qkv_bias": draw_qkv_bias(jax.random.fold_in(seeds[8], 71), 0),
        "out_weight": gaussian(seeds[5], (D, HEADS, HEAD_DIM), (HEAD_DIM * HEADS_DEV) ** -0.5, 0.375, ((0, 8),)),
        "out_bias": gaussian(seeds[6], (D,), 0.5, 3.0, ((0, 8),), jnp.float32),
        "slope_index": plant(jax.random.randint(seeds[7], (HEADS,), 0, N_SLOPES), jax.random.fold_in(seeds[7], 1), 0, N_SLOPES - 1).astype(jnp.int32),
    }


epsilon = 1e-05

def slope_values(slope_index):
    power = 1 << N_SLOPES.bit_length() - 1
    index_float = slope_index.astype(jnp.float32)
    leading = jnp.exp2(-8.0 * (index_float + 1.0) / power)
    between = jnp.exp2(-4.0 * (2.0 * (index_float - power) + 1.0) / power)
    return jnp.where(slope_index < power, leading, between)

def layer_norm(hidden, ln_gain, ln_shift):
    inputs_f32 = hidden.astype(jnp.float32)
    average = lax.optimization_barrier(jnp.mean(inputs_f32, axis=-1, keepdims=True))
    centred = inputs_f32 - average
    variance = lax.optimization_barrier(jnp.mean(centred * centred, axis=-1, keepdims=True))
    return (centred * lax.rsqrt(variance + epsilon) * ln_gain + ln_shift).astype(jnp.bfloat16)

def attend(qkv_heads, slopes):
    seq_rows = qkv_heads.shape[0]
    head_count = qkv_heads.shape[1]
    head_size = qkv_heads.shape[2] // 3
    query = qkv_heads[:, :, :head_size].astype(jnp.float32)
    keys = qkv_heads[:, :, head_size:2 * head_size].astype(jnp.float32)
    values = qkv_heads[:, :, 2 * head_size:].astype(jnp.float32)
    scores = jnp.einsum('sha,tha->hst', query, keys) / math.sqrt(head_size)
    position = jnp.arange(seq_rows, dtype=jnp.int32)
    distance = (position[:, None] - position[None, :]).astype(jnp.float32)
    scores = scores - slopes[:, None, None] * distance
    scores = jnp.where(distance >= 0.0, scores, -1e+30)
    highest = lax.optimization_barrier(jnp.max(scores, axis=-1, keepdims=True))
    powered = jnp.exp(scores - highest)
    attention = (powered / lax.optimization_barrier(jnp.sum(powered, axis=-1, keepdims=True))).astype(jnp.bfloat16)
    context = jnp.einsum('hst,tha->sha', attention.astype(jnp.float32), values).astype(jnp.bfloat16)
    return context.reshape(seq_rows, head_count * head_size)

def reference(hidden, ln_gain, ln_shift, qkv_weight, qkv_bias, out_weight, out_bias, slope_index):
    normed = layer_norm(hidden, ln_gain, ln_shift)
    projected = jnp.dot(normed, qkv_weight.reshape(D, HEADS * 3 * HEAD_DIM), preferred_element_type=jnp.float32)
    qkv = (projected.reshape(TOKENS, HEADS, 3 * HEAD_DIM) + qkv_bias).astype(jnp.bfloat16)
    slopes = slope_values(slope_index)
    context = jnp.concatenate([attend(qkv[prompt * SEQ:(prompt + 1) * SEQ], slopes) for prompt in range(N_REP)], axis=0)
    out_matrix = out_weight.reshape(D, HEADS * HEAD_DIM)
    group_width = HEADS_DEV * HEAD_DIM
    running = jnp.zeros((TOKENS, D), jnp.float32)
    for group in range(HEADS // HEADS_DEV):
        context_part = context[:, group * group_width:(group + 1) * group_width]
        weight_part = out_matrix[:, group * group_width:(group + 1) * group_width]
        partial_value = lax.dot_general(context_part, weight_part, (((1,), (1,)), ((), ())), preferred_element_type=jnp.float32).astype(jnp.bfloat16)
        partial_value = lax.optimization_barrier(partial_value)
        running = running + partial_value.astype(jnp.float32)
    return (running + out_bias).astype(jnp.bfloat16)
```

```python
import functools
import math

import jax
import jax.numpy as jnp
from jax import lax
from jax.experimental import pallas as pl
from jax.experimental.pallas import tpu as pltpu
from jax.sharding import PartitionSpec as P

N_SLOPES = 112
MESH = pl.DeviceIdType.MESH

epsilon = 1e-05


def slope_values(slope_index):
    power = 1 << N_SLOPES.bit_length() - 1
    index_float = slope_index.astype(jnp.float32)
    leading = jnp.exp2(-8.0 * (index_float + 1.0) / power)
    between = jnp.exp2(-4.0 * (2.0 * (index_float - power) + 1.0) / power)
    return jnp.where(slope_index < power, leading, between)


def fused(
    R, T, hidden, gain, shift, weight, bias, slopes, out,
    hid, nsend, xb, wv, psend, precv, acc, ctx,
    lsem, wsend, wrecv, xsend, xrecv, fsend, frecv, psends, precvs, csend, crecv, gsend, grecv,
):
    r = lax.axis_index("rep")
    t = lax.axis_index("tp")
    core = lax.rem(t, 2)
    partner = t + 1 - 2 * core
    heads, depth = weight.shape[1], weight.shape[2]
    half = hid.shape[0]
    seq = 2 * half
    width = xb.shape[2]
    total = R * width
    size = bias.shape[2] // 3
    chips = T // 2
    mine = pl.ds(pl.multiple_of(core * half, half), half)

    load = pltpu.make_async_copy(hidden.at[mine, :], hid, lsem.at[0])
    load.start()

    barrier = pltpu.get_barrier_semaphore()
    for k in range(1, T):
        pl.semaphore_signal(barrier, inc=1, device_id={"tp": lax.rem(t + k, T)}, device_id_type=MESH)
    for j in range(1, R):
        pl.semaphore_signal(barrier, inc=1, device_id={"rep": lax.rem(r + j, R)}, device_id_type=MESH)
    pl.semaphore_wait(barrier, T + R - 2)

    own_rows = pl.ds(pl.multiple_of(t * depth, 16), depth)

    def weight_copy(h, k):
        peer = lax.rem(t + k + 1, T)
        return pltpu.make_async_remote_copy(
            src_ref=weight.at[peer, h],
            dst_ref=wv.at[h, own_rows, :],
            send_sem=wsend.at[h, k],
            recv_sem=wrecv.at[h, k],
            device_id={"tp": peer},
            device_id_type=MESH,
        )

    def own_weight(h):
        return pltpu.make_async_copy(weight.at[t, h], wv.at[h, own_rows, :], lsem.at[2 + h])

    for h in range(heads):
        for k in range(T - 1):
            weight_copy(h, k).start()
        own_weight(h).start()

    load.wait()
    block = 16

    def norm_rows(i, carry):
        rows = pl.ds(pl.multiple_of(i * block, block), block)
        summed = jnp.zeros((block, 1), jnp.float32)
        for q in range(R):
            piece = hid[rows, q * width : (q + 1) * width].astype(jnp.float32)
            summed += jnp.sum(piece, axis=-1, keepdims=True)
        average = summed / total
        squares = jnp.zeros((block, 1), jnp.float32)
        for q in range(R):
            piece = hid[rows, q * width : (q + 1) * width].astype(jnp.float32) - average
            squares += jnp.sum(piece * piece, axis=-1, keepdims=True)
        scale = lax.rsqrt(squares / total + epsilon)
        for q in range(R):
            cols = slice(q * width, (q + 1) * width)
            piece = hid[rows, cols].astype(jnp.float32) - average
            nsend[q, rows, :] = (piece * scale * gain[:, cols] + shift[:, cols]).astype(jnp.bfloat16)
        return carry

    lax.fori_loop(0, half // block, norm_rows, 0)

    def norm_copy(j):
        peer = lax.rem(r + j + 1, R)
        return pltpu.make_async_remote_copy(
            src_ref=nsend.at[peer],
            dst_ref=xb.at[r, mine, :],
            send_sem=xsend.at[j],
            recv_sem=xrecv.at[j],
            device_id={"rep": peer},
            device_id_type=MESH,
        )

    def forward(j):
        owner = lax.rem(r + R - 1 - j, R)
        return pltpu.make_async_remote_copy(
            src_ref=xb.at[owner, mine, :],
            dst_ref=xb.at[owner, mine, :],
            send_sem=fsend.at[j],
            recv_sem=frecv.at[j],
            device_id={"tp": partner},
            device_id_type=MESH,
        )

    for j in range(R - 1):
        norm_copy(j).start()
    own_norm = pltpu.make_async_copy(nsend.at[r], xb.at[r, mine, :], lsem.at[1])
    own_norm.start()
    own_norm.wait()
    forward(R - 1).start()
    for j in range(R - 1):
        norm_copy(j).wait_recv()
        forward(j).start()

    def partial_copy(h, j):
        owner = lax.rem(r + R - 1 - j, R)
        return pltpu.make_async_remote_copy(
            src_ref=psend.at[h, j],
            dst_ref=precv.at[h, j],
            send_sem=psends.at[h, j],
            recv_sem=precvs.at[h, j],
            device_id={"rep": owner},
            device_id_type=MESH,
        )

    for h in range(heads):
        own_weight(h).wait()
        for k in range(T - 1):
            weight_copy(h, k).wait_recv()

        def project(j, carry, h=h):
            owner = lax.rem(r + R - 1 - j, R)
            if h == 0:
                forward(j).wait_recv()
            product = jnp.dot(xb[owner], wv[h], preferred_element_type=jnp.float32)

            @pl.when(j < R - 1)
            def _():
                psend[h, j] = product.astype(jnp.bfloat16)
                partial_copy(h, j).start()

            @pl.when(j == R - 1)
            def _():
                acc[h] = product

            return carry

        lax.fori_loop(0, R, project, 0)

    def context_cols(source, h):
        return pl.ds(pl.multiple_of(source * (heads * size) + h * size, size), size)

    def context_copy(h, k):
        peer = lax.rem(t + 2 * k + 2, T)
        cols = context_cols(t, h)
        return pltpu.make_async_remote_copy(
            src_ref=ctx.at[:, cols],
            dst_ref=ctx.at[:, cols],
            send_sem=csend.at[h, k],
            recv_sem=crecv.at[h, k],
            device_id={"tp": peer},
            device_id_type=MESH,
        )

    def context_forward(h, k):
        source = lax.rem(t + T - 2 * k, T)
        cols = context_cols(source, h)
        return pltpu.make_async_remote_copy(
            src_ref=ctx.at[:, cols],
            dst_ref=ctx.at[:, cols],
            send_sem=gsend.at[h, k],
            recv_sem=grecv.at[h, k],
            device_id={"tp": partner},
            device_id_type=MESH,
        )

    for h in range(heads):
        for j in range(R - 1):
            partial_copy(h, j).wait_recv()
        joined = acc[h]
        for j in range(R - 1):
            joined += precv[h, j].astype(jnp.float32)
        qkv = (joined + bias[h]).astype(jnp.bfloat16)
        keys = qkv[:, size : 2 * size]
        values = qkv[:, 2 * size :]
        step = min(seq, 128)
        for b in range(seq // step):
            query = qkv[b * step : (b + 1) * step, :size]
            scores = lax.dot_general(
                query, keys, (((1,), (1,)), ((), ())), preferred_element_type=jnp.float32
            ) * (1.0 / math.sqrt(size))
            distance = (
                lax.broadcasted_iota(jnp.int32, (step, seq), 0)
                + b * step
                - lax.broadcasted_iota(jnp.int32, (step, seq), 1)
            )
            scores = scores - slopes[h] * distance.astype(jnp.float32)
            scores = jnp.where(distance >= 0, scores, -1e30)
            highest = jnp.max(scores, axis=-1, keepdims=True)
            powered = jnp.exp(scores - highest)
            attention = (powered / jnp.sum(powered, axis=-1, keepdims=True)).astype(jnp.bfloat16)
            context = jnp.dot(attention, values, preferred_element_type=jnp.float32)
            ctx[b * step : (b + 1) * step, context_cols(t, h)] = context.astype(jnp.bfloat16)
        for k in range(chips - 1):
            context_copy(h, k).start()
        context_forward(h, 0).start()

    for h in range(heads):
        for k in range(1, chips):
            context_copy(h, k - 1).wait_recv()
            context_forward(h, k).start()
    for h in range(heads):
        for k in range(chips):
            context_forward(h, k).wait_recv()
    out[...] = ctx[...]

    for j in range(R):
        forward(j).wait_send()
    for j in range(R - 1):
        norm_copy(j).wait_send()
    for h in range(heads):
        for k in range(T - 1):
            weight_copy(h, k).wait_send()
        for j in range(R - 1):
            partial_copy(h, j).wait_send()
        for k in range(chips - 1):
            context_copy(h, k).wait_send()
        for k in range(chips):
            context_forward(h, k).wait_send()


def shards(hidden, ln_gain, ln_shift, qkv_weight, qkv_bias, out_weight, out_bias, slope_index):
    R, T = lax.axis_size("rep"), lax.axis_size("tp")
    seq, total = hidden.shape
    heads, wide = qkv_bias.shape
    size = wide // 3
    depth = qkv_weight.shape[0]
    width = total // R
    half = seq // 2
    chips = T // 2
    grouped = qkv_weight.reshape(depth, T, heads, wide).transpose(1, 2, 0, 3)
    vmem = pl.BlockSpec(memory_space=pltpu.VMEM)
    hbm = pl.BlockSpec(memory_space=pl.ANY)
    dma = pltpu.SemaphoreType.DMA
    context = pl.pallas_call(
        functools.partial(fused, R, T),
        out_shape=jax.ShapeDtypeStruct((seq, T * heads * size), jnp.bfloat16),
        in_specs=[hbm, vmem, vmem, hbm, vmem, pl.BlockSpec(memory_space=pltpu.SMEM)],
        out_specs=vmem,
        scratch_shapes=[
            pltpu.VMEM((half, total), jnp.bfloat16),
            pltpu.VMEM((R, half, width), jnp.bfloat16),
            pltpu.VMEM((R, seq, width), jnp.bfloat16),
            pltpu.VMEM((heads, width, wide), jnp.bfloat16),
            pltpu.VMEM((heads, R - 1, seq, wide), jnp.bfloat16),
            pltpu.VMEM((heads, R - 1, seq, wide), jnp.bfloat16),
            pltpu.VMEM((heads, seq, wide), jnp.float32),
            pltpu.VMEM((seq, T * heads * size), jnp.bfloat16),
            dma((2 + heads,)),
            dma((heads, T - 1)),
            dma((heads, T - 1)),
            dma((R - 1,)),
            dma((R - 1,)),
            dma((R,)),
            dma((R,)),
            dma((heads, R - 1)),
            dma((heads, R - 1)),
            dma((heads, chips - 1)),
            dma((heads, chips - 1)),
            dma((heads, chips)),
            dma((heads, chips)),
        ],
        compiler_params=pltpu.CompilerParams(
            collective_id=0, has_side_effects=True, vmem_limit_bytes=62 * 1024 * 1024
        ),
    )(
        hidden,
        ln_gain.reshape(1, total),
        ln_shift.reshape(1, total),
        grouped,
        qkv_bias.reshape(heads, 1, wide),
        slope_values(slope_index),
    )
    flat = out_weight.reshape(out_weight.shape[0], -1)
    result = lax.dot_general(
        context, flat, (((1,), (1,)), ((), ())), preferred_element_type=jnp.float32
    )
    return (result + out_bias).astype(jnp.bfloat16)


def solution(mesh):
    return jax.shard_map(
        shards,
        mesh=mesh,
        in_specs=(
            P("rep", None),
            P(),
            P(),
            P(("rep", "tp"), None, None),
            P("tp", None),
            P("tp", None, None),
            P("tp"),
            P("tp"),
        ),
        out_specs=P("rep", "tp"),
        check_vma=False,
    )
```

```python
import functools
import math

import jax
import jax.numpy as jnp
from jax import lax
from jax.experimental import pallas as pl
from jax.experimental.pallas import tpu as pltpu
from jax.sharding import PartitionSpec as P

N_SLOPES = 112
MESH = pl.DeviceIdType.MESH

epsilon = 1e-05


def slope_values(slope_index):
    power = 1 << N_SLOPES.bit_length() - 1
    index_float = slope_index.astype(jnp.float32)
    leading = jnp.exp2(-8.0 * (index_float + 1.0) / power)
    between = jnp.exp2(-4.0 * (2.0 * (index_float - power) + 1.0) / power)
    return jnp.where(slope_index < power, leading, between)


def fused(
    R, T, C, pieces, hidden, gain, shift, weight, bias, slope_index, out,
    hid, nsend, xb, psend, precv, acc, att, ctx, wv,
    lsem, osem, wsend, wrecv, xsend, xrecv, fsend, frecv, psends, precvs, csend, crecv, gsend, grecv,
):
    r = lax.axis_index("rep")
    t = lax.axis_index("tp")
    core = lax.rem(t, 2)
    partner = t + 1 - 2 * core
    heads, depth = weight.shape[1], weight.shape[2]
    half = hid.shape[0]
    seq = 2 * half
    width = xb.shape[2]
    total = R * width
    size = bias.shape[1] // 3
    chips = T // 2
    part = half // C
    mine = pl.ds(pl.multiple_of(core * half, half), half)

    def part_rows(c):
        return pl.ds(c * part, part)

    def part_mine(c):
        return pl.ds(pl.multiple_of(core * half + c * part, part), part)

    def load(c):
        return pltpu.make_async_copy(hidden.at[part_mine(c), :], hid.at[part_rows(c), :], lsem.at[c])

    for c in range(C):
        load(c).start()

    barrier = pltpu.get_barrier_semaphore()
    for k in range(1, T):
        pl.semaphore_signal(barrier, inc=1, device_id={"tp": lax.rem(t + k, T)}, device_id_type=MESH)
    for j in range(1, R):
        pl.semaphore_signal(barrier, inc=1, device_id={"rep": lax.rem(r + j, R)}, device_id_type=MESH)
    pl.semaphore_wait(barrier, T + R - 2)

    own_rows = pl.ds(pl.multiple_of(t * depth, 16), depth)

    def weight_copy(p, k):
        h, first, count = pieces[p]
        peer = lax.rem(t + k + 1, T)
        return pltpu.make_async_remote_copy(
            src_ref=weight.at[peer, h, :, pl.ds(first, count)],
            dst_ref=wv.at[h, own_rows, pl.ds(first, count)],
            send_sem=wsend.at[p, k],
            recv_sem=wrecv.at[p, k],
            device_id={"tp": peer},
            device_id_type=MESH,
        )

    def own_weight(h):
        return pltpu.make_async_copy(weight.at[t, h], wv.at[h, own_rows, :], osem.at[h])

    for p in range(len(pieces)):
        for k in range(T - 1):
            weight_copy(p, k).start()
    for h in range(heads):
        own_weight(h).start()

    def norm_copy(j, c):
        peer = lax.rem(r + j + 1, R)
        return pltpu.make_async_remote_copy(
            src_ref=nsend.at[peer, part_rows(c), :],
            dst_ref=xb.at[r, part_mine(c), :],
            send_sem=xsend.at[j, c],
            recv_sem=xrecv.at[j, c],
            device_id={"rep": peer},
            device_id_type=MESH,
        )

    def forward(j, c):
        owner = lax.rem(r + R - 1 - j, R)
        source = xb.at[owner, part_mine(c), :]
        if j == R - 1:
            source = nsend.at[r, part_rows(c), :]
        return pltpu.make_async_remote_copy(
            src_ref=source,
            dst_ref=xb.at[owner, part_mine(c), :],
            send_sem=fsend.at[j, c],
            recv_sem=frecv.at[j, c],
            device_id={"tp": partner},
            device_id_type=MESH,
        )

    def own_norm(c):
        return pltpu.make_async_copy(
            nsend.at[r, part_rows(c), :], xb.at[r, part_mine(c), :], lsem.at[C + c]
        )

    block = 16

    def norm_rows(i, carry):
        rows = pl.ds(pl.multiple_of(i * block, block), block)
        summed = jnp.zeros((block, 1), jnp.float32)
        for q in range(R):
            piece = hid[rows, q * width : (q + 1) * width].astype(jnp.float32)
            summed += jnp.sum(piece, axis=-1, keepdims=True)
        average = summed / total
        squares = jnp.zeros((block, 1), jnp.float32)
        for q in range(R):
            piece = hid[rows, q * width : (q + 1) * width].astype(jnp.float32) - average
            squares += jnp.sum(piece * piece, axis=-1, keepdims=True)
        scale = lax.rsqrt(squares / total + epsilon)
        for q in range(R):
            cols = slice(q * width, (q + 1) * width)
            piece = hid[rows, cols].astype(jnp.float32) - average
            nsend[q, rows, :] = (piece * scale * gain[:, cols] + shift[:, cols]).astype(jnp.bfloat16)
        return carry

    for c in range(C):
        load(c).wait()
        lax.fori_loop(c * part // block, (c + 1) * part // block, norm_rows, 0)
        for j in range(R - 1):
            norm_copy(j, c).start()
        own_norm(c).start()
        forward(R - 1, c).start()
    for c in range(C):
        for j in range(R - 1):
            norm_copy(j, c).wait_recv()
            forward(j, c).start()
    for c in range(C):
        own_norm(c).wait()
        for j in range(R):
            forward(j, c).wait_recv()

    def partial_copy(p, j):
        h, first, count = pieces[p]
        owner = lax.rem(r + R - 1 - j, R)
        return pltpu.make_async_remote_copy(
            src_ref=psend.at[h, j, :, pl.ds(first, count)],
            dst_ref=precv.at[h, j, :, pl.ds(first, count)],
            send_sem=psends.at[p, j],
            recv_sem=precvs.at[p, j],
            device_id={"rep": owner},
            device_id_type=MESH,
        )

    def project_piece(p):
        h, first, count = pieces[p]
        cols = slice(first, first + count)

        def project(j, carry):
            owner = lax.rem(r + R - 1 - j, R)
            product = jnp.dot(xb[owner], wv[h, :, cols], preferred_element_type=jnp.float32)

            @pl.when(j < R - 1)
            def _():
                psend[h, j, :, cols] = product.astype(jnp.bfloat16)
                partial_copy(p, j).start()

            @pl.when(j == R - 1)
            def _():
                acc[h, :, cols] = product

            return carry

        lax.fori_loop(0, R, project, 0)

    def wait_weight(p):
        if pieces[p][1] == 0:
            own_weight(pieces[p][0]).wait()
        for k in range(T - 1):
            weight_copy(p, k).wait_recv()

    def joined(h, first, count):
        cols = slice(first, first + count)
        result = acc[h, :, cols]
        for j in range(R - 1):
            result += precv[h, j, :, cols].astype(jnp.float32)
        return (result + bias[h : h + 1, cols]).astype(jnp.bfloat16)

    def context_cols(source, h):
        return pl.ds(pl.multiple_of(source * (heads * size) + h * size, size), size)

    def context_copy(h, k):
        peer = lax.rem(t + 2 * k + 2, T)
        cols = context_cols(t, h)
        return pltpu.make_async_remote_copy(
            src_ref=ctx.at[:, cols],
            dst_ref=ctx.at[:, cols],
            send_sem=csend.at[h, k],
            recv_sem=crecv.at[h, k],
            device_id={"tp": peer},
            device_id_type=MESH,
        )

    def context_forward(h, k):
        source = lax.rem(t + T - 2 * k, T)
        cols = context_cols(source, h)
        return pltpu.make_async_remote_copy(
            src_ref=ctx.at[:, cols],
            dst_ref=ctx.at[:, cols],
            send_sem=gsend.at[h, k],
            recv_sem=grecv.at[h, k],
            device_id={"tp": partner},
            device_id_type=MESH,
        )

    def attend(h):
        both = joined(h, 0, 2 * size)
        keys = both[:, size:]
        index = jnp.full((1, seq), slope_index[h], jnp.int32)
        slope = slope_values(index)
        step = min(seq, 128)
        for b in range(seq // step):
            query = both[b * step : (b + 1) * step, :size]
            scores = lax.dot_general(
                query, keys, (((1,), (1,)), ((), ())), preferred_element_type=jnp.float32
            ) * (1.0 / math.sqrt(size))
            distance = (
                lax.broadcasted_iota(jnp.int32, (step, seq), 0)
                + b * step
                - lax.broadcasted_iota(jnp.int32, (step, seq), 1)
            )
            scores = scores - slope * distance.astype(jnp.float32)
            scores = jnp.where(distance >= 0, scores, -1e30)
            highest = jnp.max(scores, axis=-1, keepdims=True)
            powered = jnp.exp(scores - highest)
            att[b * step : (b + 1) * step, :] = (
                powered / jnp.sum(powered, axis=-1, keepdims=True)
            ).astype(jnp.bfloat16)

    def combine(h):
        values = joined(h, 2 * size, size)
        context = jnp.dot(att[...], values, preferred_element_type=jnp.float32)
        ctx[:, context_cols(t, h)] = context.astype(jnp.bfloat16)

    def send_context(h):
        for k in range(chips - 1):
            context_copy(h, k).start()
        context_forward(h, 0).start()

    last = len(pieces) - 1
    for p in range(last):
        wait_weight(p)
        project_piece(p)
    for p in range(last):
        for j in range(R - 1):
            partial_copy(p, j).wait_recv()
        h = pieces[p][0]
        attend(h)
        if p < last - 1:
            combine(h)
    wait_weight(last)
    for h in range(heads - 1):
        send_context(h)
    project_piece(last)
    for j in range(R - 1):
        partial_copy(last, j).wait_recv()
    combine(heads - 1)
    send_context(heads - 1)

    for h in range(heads):
        for k in range(1, chips):
            context_copy(h, k - 1).wait_recv()
            context_forward(h, k).start()
    for h in range(heads):
        for k in range(chips):
            context_forward(h, k).wait_recv()
    out[...] = ctx[...]

    for c in range(C):
        for j in range(R):
            forward(j, c).wait_send()
        for j in range(R - 1):
            norm_copy(j, c).wait_send()
    for p in range(len(pieces)):
        for k in range(T - 1):
            weight_copy(p, k).wait_send()
        for j in range(R - 1):
            partial_copy(p, j).wait_send()
    for h in range(heads):
        for k in range(chips - 1):
            context_copy(h, k).wait_send()
        for k in range(chips):
            context_forward(h, k).wait_send()


def shards(hidden, ln_gain, ln_shift, qkv_weight, qkv_bias, out_weight, out_bias, slope_index):
    R, T = lax.axis_size("rep"), lax.axis_size("tp")
    seq, total = hidden.shape
    heads, wide = qkv_bias.shape
    size = wide // 3
    depth = qkv_weight.shape[0]
    width = total // R
    half = seq // 2
    chips = T // 2
    C = 4
    pieces = [(h, 0, wide) for h in range(heads - 1)]
    pieces += [(heads - 1, 0, 2 * size), (heads - 1, 2 * size, size)]
    count = len(pieces)
    grouped = qkv_weight.reshape(depth, T, heads, wide).transpose(1, 2, 0, 3)
    vmem = pl.BlockSpec(memory_space=pltpu.VMEM)
    hbm = pl.BlockSpec(memory_space=pl.ANY)
    dma = pltpu.SemaphoreType.DMA
    context = pl.pallas_call(
        functools.partial(fused, R, T, C, pieces),
        out_shape=jax.ShapeDtypeStruct((seq, T * heads * size), jnp.bfloat16),
        in_specs=[hbm, vmem, vmem, hbm, vmem, pl.BlockSpec(memory_space=pltpu.SMEM)],
        out_specs=vmem,
        scratch_shapes=[
            pltpu.VMEM((half, total), jnp.bfloat16),
            pltpu.VMEM((R, half, width), jnp.bfloat16),
            pltpu.VMEM((R, seq, width), jnp.bfloat16),
            pltpu.VMEM((heads, R - 1, seq, wide), jnp.bfloat16),
            pltpu.VMEM((heads, R - 1, seq, wide), jnp.bfloat16),
            pltpu.VMEM((heads, seq, wide), jnp.float32),
            pltpu.VMEM((seq, seq), jnp.bfloat16),
            pltpu.VMEM((seq, T * heads * size), jnp.bfloat16),
            pltpu.VMEM((heads, width, wide), jnp.bfloat16),
            dma((2 * C,)),
            dma((heads,)),
            dma((count, T - 1)),
            dma((count, T - 1)),
            dma((R - 1, C)),
            dma((R - 1, C)),
            dma((R, C)),
            dma((R, C)),
            dma((count, R - 1)),
            dma((count, R - 1)),
            dma((heads, chips - 1)),
            dma((heads, chips - 1)),
            dma((heads, chips)),
            dma((heads, chips)),
        ],
        compiler_params=pltpu.CompilerParams(
            collective_id=0, has_side_effects=True, vmem_limit_bytes=62 * 1024 * 1024
        ),
    )(
        hidden,
        ln_gain.reshape(1, total),
        ln_shift.reshape(1, total),
        grouped,
        qkv_bias,
        slope_index,
    )
    flat = out_weight.reshape(out_weight.shape[0], -1)
    result = lax.dot_general(
        context, flat, (((1,), (1,)), ((), ())), preferred_element_type=jnp.float32
    )
    return (result + out_bias).astype(jnp.bfloat16)


def solution(mesh):
    return jax.shard_map(
        shards,
        mesh=mesh,
        in_specs=(
            P("rep", None),
            P(),
            P(),
            P(("rep", "tp"), None, None),
            P("tp", None),
            P("tp", None, None),
            P("tp"),
            P("tp"),
        ),
        out_specs=P("rep", "tp"),
        check_vma=False,
    )
```

```python
import functools
import math

import jax
import jax.numpy as jnp
from jax import lax
from jax.experimental import pallas as pl
from jax.experimental.pallas import tpu as pltpu
from jax.sharding import PartitionSpec as P

N_SLOPES = 112
MESH = pl.DeviceIdType.MESH

epsilon = 1e-05


def slope_values(slope_index):
    power = 1 << N_SLOPES.bit_length() - 1
    index_float = slope_index.astype(jnp.float32)
    leading = jnp.exp2(-8.0 * (index_float + 1.0) / power)
    between = jnp.exp2(-4.0 * (2.0 * (index_float - power) + 1.0) / power)
    return jnp.where(slope_index < power, leading, between)


def fused(
    R, T, C, pieces, parts, units, hidden, gain, shift, weight, bias, slope_index, proj, out, flat,
    hid, nsend, xb, psend, precv, acc, att, ctx, wv, vals, stage, staged,
    isem, jsem, lsem, osem, wsend, wrecv, xsend, xrecv, fsend, frecv, psends, precvs, csend, crecv, gsend, grecv,
):
    r = lax.axis_index("rep")
    t = lax.axis_index("tp")
    core = lax.rem(t, 2)
    partner = t + 1 - 2 * core
    heads, depth = wv.shape[0], weight.shape[2]
    half = hid.shape[0]
    seq = 2 * half
    width = xb.shape[2]
    total = R * width
    size = bias.shape[1] // 3
    chips = T // 2
    part = half // C
    mine = pl.ds(pl.multiple_of(core * half, half), half)

    def part_rows(c):
        return pl.ds(c * part, part)

    def part_mine(c):
        return pl.ds(pl.multiple_of(core * half + c * part, part), part)

    def load(c):
        return pltpu.make_async_copy(hidden.at[part_mine(c), :], hid.at[part_rows(c), :], lsem.at[c])

    for c in range(C):
        load(c).start()

    chunk = stage.shape[1]

    def stage_in(i):
        rows = pl.ds(i * chunk, chunk)
        return pltpu.make_async_copy(proj.at[rows], stage.at[i % 2], isem.at[i % 2])

    def stage_out(i):
        rows = pl.ds(i * chunk, chunk)
        return pltpu.make_async_copy(staged.at[i % 2], flat.at[rows, :], jsem.at[i % 2])

    for i in range(2):
        stage_in(i).start()

    barrier = pltpu.get_barrier_semaphore()
    for k in range(1, T):
        pl.semaphore_signal(barrier, inc=1, device_id={"tp": lax.rem(t + k, T)}, device_id_type=MESH)
    for j in range(1, R):
        pl.semaphore_signal(barrier, inc=1, device_id={"rep": lax.rem(r + j, R)}, device_id_type=MESH)
    pl.semaphore_wait(barrier, T + R - 2)

    own_rows = pl.ds(pl.multiple_of(t * depth, 16), depth)

    def weight_copy(p, k):
        h, first, count = pieces[p]
        peer = lax.rem(t + k + 1, T)
        return pltpu.make_async_remote_copy(
            src_ref=weight.at[peer, h, :, pl.ds(first, count)],
            dst_ref=wv.at[h, own_rows, pl.ds(first, count)],
            send_sem=wsend.at[p, k],
            recv_sem=wrecv.at[p, k],
            device_id={"tp": peer},
            device_id_type=MESH,
        )

    def own_weight(h):
        return pltpu.make_async_copy(weight.at[t, h], wv.at[h, own_rows, :], osem.at[h])

    for h in range(heads):
        for p in range(len(pieces)):
            if pieces[p][0] == h:
                for k in range(T - 1):
                    weight_copy(p, k).start()
        own_weight(h).start()

    def norm_copy(j, c):
        peer = lax.rem(r + j + 1, R)
        return pltpu.make_async_remote_copy(
            src_ref=nsend.at[peer, part_rows(c), :],
            dst_ref=xb.at[r, part_mine(c), :],
            send_sem=xsend.at[j, c],
            recv_sem=xrecv.at[j, c],
            device_id={"rep": peer},
            device_id_type=MESH,
        )

    def forward(j, c):
        owner = lax.rem(r + R - 1 - j, R)
        source = xb.at[owner, part_mine(c), :]
        if j == R - 1:
            source = nsend.at[r, part_rows(c), :]
        return pltpu.make_async_remote_copy(
            src_ref=source,
            dst_ref=xb.at[owner, part_mine(c), :],
            send_sem=fsend.at[j, c],
            recv_sem=frecv.at[j, c],
            device_id={"tp": partner},
            device_id_type=MESH,
        )

    def own_norm(c):
        return pltpu.make_async_copy(
            nsend.at[r, part_rows(c), :], xb.at[r, part_mine(c), :], lsem.at[C + c]
        )

    block = 16

    def norm_rows(i, carry):
        rows = pl.ds(pl.multiple_of(i * block, block), block)
        summed = jnp.zeros((block, 1), jnp.float32)
        for q in range(R):
            piece = hid[rows, q * width : (q + 1) * width].astype(jnp.float32)
            summed += jnp.sum(piece, axis=-1, keepdims=True)
        average = summed / total
        squares = jnp.zeros((block, 1), jnp.float32)
        for q in range(R):
            piece = hid[rows, q * width : (q + 1) * width].astype(jnp.float32) - average
            squares += jnp.sum(piece * piece, axis=-1, keepdims=True)
        scale = lax.rsqrt(squares / total + epsilon)
        for q in range(R):
            cols = slice(q * width, (q + 1) * width)
            piece = hid[rows, cols].astype(jnp.float32) - average
            nsend[q, rows, :] = (piece * scale * gain[:, cols] + shift[:, cols]).astype(jnp.bfloat16)
        return carry

    for c in range(C):
        load(c).wait()
        lax.fori_loop(c * part // block, (c + 1) * part // block, norm_rows, 0)
        for j in range(R - 1):
            norm_copy(j, c).start()
        own_norm(c).start()
        forward(R - 1, c).start()

    steps = proj.shape[0] // chunk
    for i in range(steps):
        stage_in(i).wait()
        if i >= 2:
            stage_out(i - 2).wait()

        def flatten(b, carry, slot=i % 2):
            rows = pl.ds(pl.multiple_of(b * 16, 16), 16)
            for g in range(proj.shape[1]):
                staged[slot, rows, g * size : (g + 1) * size] = stage[slot, rows, g, :]
            return carry

        lax.fori_loop(0, chunk // 16, flatten, 0)
        stage_out(i).start()
        if i + 2 < steps:
            stage_in(i + 2).start()
    for i in range(max(steps - 2, 0), steps):
        stage_out(i).wait()

    for c in range(C):
        for j in range(R - 1):
            norm_copy(j, c).wait_recv()
            forward(j, c).start()
    for c in range(C):
        own_norm(c).wait()
        for j in range(R):
            forward(j, c).wait_recv()

    def partial_copy(q, j):
        h, first, count, top, tall = parts[q]
        owner = lax.rem(r + R - 1 - j, R)
        area = (h, j, pl.ds(top, tall), pl.ds(first, count))
        return pltpu.make_async_remote_copy(
            src_ref=psend.at[area],
            dst_ref=precv.at[area],
            send_sem=psends.at[q, j],
            recv_sem=precvs.at[q, j],
            device_id={"rep": owner},
            device_id_type=MESH,
        )

    def project_part(q):
        h, first, count, top, tall = parts[q]
        cols = slice(first, first + count)
        rows = slice(top, top + tall)

        def project(j, carry):
            owner = lax.rem(r + R - 1 - j, R)
            product = jnp.dot(xb[owner, rows], wv[h, :, cols], preferred_element_type=jnp.float32)

            @pl.when(j < R - 1)
            def _():
                psend[h, j, rows, cols] = product.astype(jnp.bfloat16)
                partial_copy(q, j).start()

            @pl.when(j == R - 1)
            def _():
                acc[h, rows, cols] = product

            return carry

        lax.fori_loop(0, R, project, 0)

    def wait_weight(p):
        if pieces[p][1] == 0:
            own_weight(pieces[p][0]).wait()
        for k in range(T - 1):
            weight_copy(p, k).wait_recv()

    def joined(h, first, count, top, tall):
        cols = slice(first, first + count)
        rows = slice(top, top + tall)
        result = acc[h, rows, cols]
        for j in range(R - 1):
            result += precv[h, j, rows, cols].astype(jnp.float32)
        return (result + bias[h : h + 1, cols]).astype(jnp.bfloat16)

    def context_cols(source, h):
        return pl.ds(pl.multiple_of(source * (heads * size) + h * size, size), size)

    def context_copy(u, k):
        h, top, tall = units[u]
        peer = lax.rem(t + 2 * k + 2, T)
        area = (pl.ds(top, tall), context_cols(t, h))
        return pltpu.make_async_remote_copy(
            src_ref=ctx.at[area],
            dst_ref=ctx.at[area],
            send_sem=csend.at[u, k],
            recv_sem=crecv.at[u, k],
            device_id={"tp": peer},
            device_id_type=MESH,
        )

    def context_forward(u, k):
        h, top, tall = units[u]
        source = lax.rem(t + T - 2 * k, T)
        area = (pl.ds(top, tall), context_cols(source, h))
        return pltpu.make_async_remote_copy(
            src_ref=ctx.at[area],
            dst_ref=ctx.at[area],
            send_sem=gsend.at[u, k],
            recv_sem=grecv.at[u, k],
            device_id={"tp": partner},
            device_id_type=MESH,
        )

    def attend(h):
        both = joined(h, 0, 2 * size, 0, seq)
        keys = both[:, size:]
        index = jnp.full((1, seq), slope_index[h], jnp.int32)
        slope = slope_values(index)
        step = min(seq, 128)
        for b in range(seq // step):
            query = both[b * step : (b + 1) * step, :size]
            scores = lax.dot_general(
                query, keys, (((1,), (1,)), ((), ())), preferred_element_type=jnp.float32
            ) * (1.0 / math.sqrt(size))
            distance = (
                lax.broadcasted_iota(jnp.int32, (step, seq), 0)
                + b * step
                - lax.broadcasted_iota(jnp.int32, (step, seq), 1)
            )
            scores = scores - slope * distance.astype(jnp.float32)
            scores = jnp.where(distance >= 0, scores, -1e30)
            highest = jnp.max(scores, axis=-1, keepdims=True)
            powered = jnp.exp(scores - highest)
            att[b * step : (b + 1) * step, :] = (
                powered / jnp.sum(powered, axis=-1, keepdims=True)
            ).astype(jnp.bfloat16)

    def combine(u):
        h, top, tall = units[u]
        rows = slice(top, top + tall)
        vals[rows, :] = joined(h, 2 * size, size, top, tall)
        reach = top + tall
        context = jnp.dot(att[rows, :reach], vals[:reach, :], preferred_element_type=jnp.float32)
        ctx[rows, context_cols(t, h)] = context.astype(jnp.bfloat16)

    def send_context(u):
        for k in range(chips - 1):
            context_copy(u, k).start()
        context_forward(u, 0).start()

    last = len(pieces) - 1
    for p in range(last):
        wait_weight(p)
        project_part(p)
    for p in range(last):
        for j in range(R - 1):
            partial_copy(p, j).wait_recv()
        attend(pieces[p][0])
        if p < last - 1:
            combine(p)
    wait_weight(last)
    for u in range(heads - 1):
        send_context(u)
    for q in range(last, len(parts)):
        project_part(q)
    for q in range(last, len(parts)):
        for j in range(R - 1):
            partial_copy(q, j).wait_recv()
        combine(q - 1)
        send_context(q - 1)

    for u in range(len(units)):
        for k in range(1, chips):
            context_copy(u, k - 1).wait_recv()
            context_forward(u, k).start()
    for u in range(len(units)):
        for k in range(chips):
            context_forward(u, k).wait_recv()
    result = pltpu.make_async_copy(ctx, out, lsem.at[0])
    result.start()

    for c in range(C):
        for j in range(R):
            forward(j, c).wait_send()
        for j in range(R - 1):
            norm_copy(j, c).wait_send()
    for p in range(len(pieces)):
        for k in range(T - 1):
            weight_copy(p, k).wait_send()
    for q in range(len(parts)):
        for j in range(R - 1):
            partial_copy(q, j).wait_send()
    for u in range(len(units)):
        for k in range(chips - 1):
            context_copy(u, k).wait_send()
        for k in range(chips):
            context_forward(u, k).wait_send()
    result.wait()


def shards(hidden, ln_gain, ln_shift, qkv_weight, qkv_bias, out_weight, out_bias, slope_index):
    R, T = lax.axis_size("rep"), lax.axis_size("tp")
    seq, total = hidden.shape
    heads, wide = qkv_bias.shape
    size = wide // 3
    depth = qkv_weight.shape[0]
    width = total // R
    half = seq // 2
    chips = T // 2
    C = 4
    pieces = [(h, 0, wide) for h in range(heads - 1)]
    pieces += [(heads - 1, 0, 2 * size), (heads - 1, 2 * size, size)]
    count = len(pieces)
    parts = [piece + (0, seq) for piece in pieces[:-1]]
    parts += [pieces[-1] + (0, half), pieces[-1] + (half, half)]
    units = [(h, 0, seq) for h in range(heads - 1)]
    units += [(heads - 1, 0, half), (heads - 1, half, half)]
    chunk = math.gcd(out_weight.shape[0], 128)
    vmem = pl.BlockSpec(memory_space=pltpu.VMEM)
    hbm = pl.BlockSpec(memory_space=pl.ANY)
    dma = pltpu.SemaphoreType.DMA
    context, flat = pl.pallas_call(
        functools.partial(fused, R, T, C, pieces, parts, units),
        out_shape=(
            jax.ShapeDtypeStruct((seq, T * heads * size), jnp.bfloat16),
            jax.ShapeDtypeStruct((out_weight.shape[0], T * heads * size), jnp.bfloat16),
        ),
        in_specs=[hbm, vmem, vmem, hbm, vmem, pl.BlockSpec(memory_space=pltpu.SMEM), hbm],
        out_specs=(hbm, hbm),
        scratch_shapes=[
            pltpu.VMEM((half, total), jnp.bfloat16),
            pltpu.VMEM((R, half, width), jnp.bfloat16),
            pltpu.VMEM((R, seq, width), jnp.bfloat16),
            pltpu.VMEM((heads, R - 1, seq, wide), jnp.bfloat16),
            pltpu.VMEM((heads, R - 1, seq, wide), jnp.bfloat16),
            pltpu.VMEM((heads, seq, wide), jnp.float32),
            pltpu.VMEM((seq, seq), jnp.bfloat16),
            pltpu.VMEM((seq, T * heads * size), jnp.bfloat16),
            pltpu.VMEM((heads, width, wide), jnp.bfloat16),
            pltpu.VMEM((seq, size), jnp.bfloat16),
            pltpu.VMEM((2, chunk, T * heads, size), jnp.bfloat16),
            pltpu.VMEM((2, chunk, T * heads * size), jnp.bfloat16),
            dma((2,)),
            dma((2,)),
            dma((2 * C,)),
            dma((heads,)),
            dma((count, T - 1)),
            dma((count, T - 1)),
            dma((R - 1, C)),
            dma((R - 1, C)),
            dma((R, C)),
            dma((R, C)),
            dma((count + 1, R - 1)),
            dma((count + 1, R - 1)),
            dma((len(units), chips - 1)),
            dma((len(units), chips - 1)),
            dma((len(units), chips)),
            dma((len(units), chips)),
        ],
        compiler_params=pltpu.CompilerParams(
            collective_id=0, has_side_effects=True, vmem_limit_bytes=62 * 1024 * 1024
        ),
    )(
        hidden,
        ln_gain.reshape(1, total),
        ln_shift.reshape(1, total),
        qkv_weight.reshape(depth, T, heads, wide).transpose(1, 2, 0, 3),
        qkv_bias,
        slope_index,
        out_weight,
    )
    result = lax.dot_general(
        context, flat, (((1,), (1,)), ((), ())), preferred_element_type=jnp.float32
    )
    return (result + out_bias).astype(jnp.bfloat16)


def solution(mesh):
    return jax.shard_map(
        shards,
        mesh=mesh,
        in_specs=(
            P("rep", None),
            P(),
            P(),
            P(("rep", "tp"), None, None),
            P("tp", None),
            P("tp", None, None),
            P("tp"),
            P("tp"),
        ),
        out_specs=P("rep", "tp"),
        check_vma=False,
    )
```
